256 devices in a mesh: owner: 16 (over y, x), rows: 16 (over z, core).
Axes of the slice: x: 4, y: 4, z: 8, core: 2. Of those that a mesh axis runs over, the one named last changes fastest.
Arguments:
- train_gate: float32 [64, 2048, 1024], P('owner', 'rows'), may hold values from -0.1875 to 0.1875
- train_up: float32 [64, 2048, 1024], P('owner', 'rows'), may hold values from -0.1875 to 0.1875
- train_down: float32 [64, 1024, 2048], P('owner', None, 'rows'), may hold values from -0.25 to 0.25
- router_weight: float32 [2048, 64], P('rows', 'owner'), may hold values from -0.125 to 0.125
- router_gain: float32 [2048], P('rows'), may hold values from 0.25 to 1.75
Outputs:
- ready_gate: bfloat16 [64, 2048, 1024], P('owner', None, 'rows')
- ready_up: bfloat16 [64, 2048, 1024], P('owner', None, 'rows')
- ready_down: bfloat16 [64, 1024, 2048], P('owner', 'rows')
- scale_gate: float32 [64, 1024], P('owner', 'rows')
- scale_up: float32 [64, 1024], P('owner', 'rows')
- scale_down: float32 [64, 1024], P('owner', 'rows')
- serve_router: bfloat16 [2048, 64], replicated
The draws below stay inside these ranges and needn't reach their ends.
All inputs are finite; a program needn't handle non-finite values. Where the reference program divides by a largest or mean magnitude, that divisor is 1e-20 or more.
Results may differ from the reference program's by a relative error of at most 0.0013.
Values may be sent and summed in bfloat16 or wider, within the bound.
No kernel may reach another device: no remote copies, remote signals or barrier semaphores. Data moves between devices by JAX's collectives and lax.ppermute only.
A program may use at most 64 MiB of HBM per device.

```python
import jax
import jax.numpy as jnp

EXPERTS = 64
D_MODEL = 2048
D_EXPERT = 1024


def raised(drawn, own_key, source, target, parts, factor):
    owner, partner = [(jnp.arange(drawn.shape[axis_at]) // (drawn.shape[axis_at] // parts)).reshape([-1 if axis == axis_at else 1 for axis in range(drawn.ndim)]) for axis_at in (source, target)]
    chosen = jax.random.permutation(own_key, parts)[partner]
    strong = (owner == chosen) | (owner == (partner + parts // 2) % parts)
    return jnp.where(strong, factor * drawn, drawn)


def steps_of(rng, dims, shards, low, top_value):
    def one(dim, parts):
        heights = jax.random.uniform(jax.random.fold_in(jax.random.fold_in(rng, 6), dim), (parts,), jnp.float32, low / len(shards), top_value / len(shards))
        return jnp.repeat(jnp.exp(heights), dims[dim] // parts).reshape((-1,) + (1,) * (len(dims) - dim - 1))

    factor_of = one(*shards[0])
    for cut in shards[1:]:
        factor_of = factor_of * one(*cut)
    return factor_of


def bell_draw(own_key, shape, scale, reach, pieces=(), dtype=jnp.bfloat16):
    result = scale * jax.random.normal(own_key, shape, jnp.float32)
    if pieces:
        result = result * steps_of(own_key, shape, pieces, -0.22, 0.18)
    return jnp.clip(result, -reach, reach).astype(dtype)


def bell_draw_with(own_key, dims, deviation, reach, split, heavy, kind=jnp.bfloat16):
    result = deviation * jax.random.normal(own_key, dims, jnp.float32)
    if split:
        result = result * steps_of(own_key, dims, split, -0.22, 0.18)
    return jnp.clip(raised(result, jax.random.fold_in(own_key, 3), *heavy), -reach, reach).astype(kind)


def setup_inputs(seed: int = 0) -> dict:
    splits = jax.random.split(jax.random.key(seed), 6)
    train_gate = bell_draw_with(splits[0], (EXPERTS, D_MODEL, D_EXPERT), D_MODEL ** -0.5, 0.1875, ((0, 16), (1, 16)), (1, 2, 16, 2.0), jnp.float32)
    train_up = bell_draw_with(splits[1], (EXPERTS, D_MODEL, D_EXPERT), D_MODEL ** -0.5, 0.1875, ((0, 16), (1, 16)), (1, 2, 16, 2.0), jnp.float32)
    train_down = bell_draw_with(splits[2], (EXPERTS, D_EXPERT, D_MODEL), D_EXPERT ** -0.5, 0.25, ((0, 16), (2, 16)), (2, 1, 16, 2.0), jnp.float32)
    router_weight = bell_draw(splits[3], (D_MODEL, EXPERTS), D_MODEL ** -0.5, 0.125, ((0, 16), (1, 16)), jnp.float32)
    router_gain = jnp.clip(1.0 + 0.15 * jax.random.normal(splits[4], (D_MODEL,), jnp.float32), 0.25, 1.75)
    return {"train_gate": train_gate, "train_up": train_up, "train_down": train_down, "router_weight": router_weight, "router_gain": router_gain}


def reference(train_gate, train_up, train_down, router_weight, router_gain):
    scale_gate = jnp.sum(jnp.abs(train_gate), axis=1) / D_MODEL
    ready_gate = (train_gate / jnp.expand_dims(scale_gate, 1)).astype(jnp.bfloat16)
    scale_up = jnp.sum(jnp.abs(train_up), axis=1) / D_MODEL
    ready_up = (train_up / jnp.expand_dims(scale_up, 1)).astype(jnp.bfloat16)
    scale_down = jnp.sum(jnp.abs(train_down), axis=2) / D_MODEL
    ready_down = (train_down / jnp.expand_dims(scale_down, 2)).astype(jnp.bfloat16)
    serve_router = (router_weight * router_gain[:, None]).astype(jnp.bfloat16)
    return ready_gate, ready_up, ready_down, scale_gate, scale_up, scale_down, serve_router
```

```python
import functools

import jax
import jax.numpy as jnp
from jax import lax
from jax.experimental import pallas as pl
from jax.experimental.pallas import tpu as pltpu
from jax.sharding import PartitionSpec as P


D_MODEL = 2048
E = 4
N = 3 * E
CHIPS = 8
POWER = 13
AMP = 700.0
FLOOR = 1e-25

FIRST = (3, -3)
REST = (1, -1, 2, -2, 4, 0)
ORDER = (
    (3, 0), (-3, 0), (3, 1), (-3, 1), (1, 0), (-1, 0), (2, 0), (-2, 0),
    (4, 0), (4, 1), (2, 1), (-2, 1), (1, 1), (-1, 1), (0, 1),
)


def place():
    r = lax.axis_index("rows")
    return r // 2, r % 2


def pairs_of(dz, dc):
    return [
        (2 * z + c, 2 * ((z + dz) % CHIPS) + (c ^ dc)) for z in range(CHIPS) for c in range(2)
    ]


def code(x, sums):
    v = x * (AMP / jnp.maximum(sums, FLOOR))
    v2 = v * v
    v4 = v2 * v2
    return (v4 * v4 * v4 * v).astype(jnp.bfloat16)


def fetches(dzs, z, ins, buf, sems):
    gate, up, down = ins
    out = []
    for i, dz in enumerate(dzs):
        at = pl.ds(pl.multiple_of(lax.rem(z + (dz % CHIPS), CHIPS) * 128, 128), 128)
        out.append(
            [
                pltpu.make_async_copy(gate.at[:, :, at], buf.at[i, 0], sems.at[i, 0]),
                pltpu.make_async_copy(up.at[:, :, at], buf.at[i, 1], sems.at[i, 1]),
                pltpu.make_async_copy(down.at[:, at, :], buf.at[i, 2], sems.at[i, 2]),
            ]
        )
    return out


def encode(dzs, place_ref, ins, outs, sums, buf, sems):
    z, c = place_ref[0], place_ref[1]
    copies = fetches(dzs, z, ins, buf, sems)
    for three in copies:
        for copy in three:
            copy.start()
    diagonal = lax.broadcasted_iota(jnp.int32, (128, 128), 0) == lax.broadcasted_iota(
        jnp.int32, (128, 128), 1
    )
    mine = c == 0
    for i, three in enumerate(copies):
        same, other = outs[2 * i], outs[2 * i + 1]
        for copy in three:
            copy.wait()

        def put(n, coded):
            low, high = coded[:64], coded[64:]
            same[n] = jnp.where(mine, low, high)
            other[n] = jnp.where(mine, high, low)

        def one(e, carry):
            for a in range(2):
                x = buf[i, a, e]
                total = jnp.sum(jnp.abs(x), axis=0, keepdims=True)
                sums[i, a * E + e] = total
                put(a * E + e, code(x, total).T)
            x = buf[i, 2, e]
            total = jnp.sum(jnp.abs(x), axis=1, keepdims=True)
            sums[i, 2 * E + e] = jnp.sum(jnp.where(diagonal, total, 0.0), axis=0, keepdims=True)
            put(2 * E + e, code(x, total))
            return carry

        lax.fori_loop(0, E, one, 0)


def first_kernel(place_ref, gate, up, down, *rest):
    outs, (sums, buf, sems) = rest[: 2 * len(FIRST)], rest[2 * len(FIRST) :]
    encode(FIRST, place_ref, (gate, up, down), outs, sums, buf, sems)


def rest_kernel(place_ref, gate, up, down, early, router, gain, *rest):
    outs, (table, sums, buf, sems) = rest[: 2 * len(REST)], rest[2 * len(REST) :]
    encode(REST, place_ref, (gate, up, down), outs, sums, buf, sems)
    z = place_ref[0]
    left = lax.broadcasted_iota(jnp.int32, (1, 128), 1) < 64
    served = (router[...] * gain[...]).astype(jnp.bfloat16).astype(jnp.float32)
    for dzs, ref in ((FIRST, early), (REST, sums)):
        for i, dz in enumerate(dzs):
            chip = lax.rem(z + (dz % CHIPS), CHIPS)
            for q in range(N // 2):
                a, b = ref[i, 2 * q], ref[i, 2 * q + 1]
                at = slice(q * 128, q * 128 + 128)
                table[2 * chip, :, at] = jnp.where(left, a, pltpu.roll(b, 64, 1))
                table[2 * chip + 1, :, at] = jnp.where(left, pltpu.roll(a, 64, 1), b)
            for core in range(2):
                for q in range(4):
                    at = slice((N // 2 + q) * 128, (N // 2 + q) * 128 + 128)
                    table[2 * chip + core, :, at] = served[q : q + 1]


def scale_kernel(table, gate, up, down, factors, rows):
    total = table[0]
    for s in range(1, 16):
        total = total + table[s]
    scale = total[:, : N // 2 * 128] / D_MODEL
    for n in range(N):
        out = (gate, up, down)[n // E]
        out[n % E : n % E + 1, :] = scale[:, n * 64 : n * 64 + 64]
    for s in range(16):
        f = jnp.maximum(table[s, :, : N // 2 * 128], FLOOR) / (AMP * scale)
        f = [f[:, q * 128 : q * 128 + 128] for q in range(N // 2)]
        factors[s] = jnp.concatenate(f + f[:2], axis=0).T
        for q in range(4):
            at = slice((N // 2 + q) * 128, (N // 2 + q) * 128 + 128)
            rows[q : q + 1, s * 128 : s * 128 + 128] = table[s, :, at].astype(jnp.bfloat16)


def decode_kernel(where, n_alias, place_ref, factors, *rest):
    n = len(where)
    pieces, rest = rest[:n], rest[n + n_alias :]
    outs, (buf, sems) = rest[:3], rest[3:]
    z, c = place_ref[0], place_ref[1]
    copies = []
    for i, (dz, dc) in enumerate(where):
        s = 2 * lax.rem(z + (-dz % CHIPS), CHIPS) + (c if dc == 0 else 1 - c)
        f = factors[s]
        for k in range(N):
            w = pieces[i][k].astype(jnp.float32)
            root = jnp.exp(jnp.log(jnp.abs(w)) * (1.0 / POWER))
            root = jnp.where(w < 0, -root, root)
            half = k % 2 * 64
            buf[i, k] = (root * f[half : half + 64, k // 2 : k // 2 + 1]).astype(jnp.bfloat16)
        at = pl.ds(pl.multiple_of(s * 128, 128), 128)
        for a in range(3):
            copy = pltpu.make_async_copy(
                buf.at[i, a * E : a * E + E], outs[a].at[:, :, at], sems.at[i, a]
            )
            copy.start()
            copies.append(copy)
    for copy in copies:
        copy.wait()


SMEM = pl.BlockSpec(memory_space=pltpu.SMEM)
VMEM = pl.BlockSpec(memory_space=pltpu.VMEM)
ANY = pl.BlockSpec(memory_space=pl.ANY)
PIECE = jax.ShapeDtypeStruct((N, 64, 128), jnp.bfloat16)


def decode(where, place_, factors, pieces, before):
    n = len(where)
    out = jax.ShapeDtypeStruct((E, 64, 16 * 128), jnp.bfloat16)
    return pl.pallas_call(
        functools.partial(decode_kernel, where, len(before)),
        out_shape=(out,) * 3,
        in_specs=[SMEM, VMEM] + [VMEM] * n + [ANY] * len(before),
        out_specs=(ANY,) * 3,
        scratch_shapes=[
            pltpu.VMEM((n, N, 64, 128), jnp.bfloat16),
            pltpu.SemaphoreType.DMA((n, 3)),
        ],
        input_output_aliases={2 + n + a: a for a in range(len(before))},
        cost_estimate=pl.CostEstimate(
            flops=n * 10_000_000, transcendentals=0, bytes_accessed=n * 400_000
        ),
    )(place_, factors, *pieces, *before)


GROUPS = (
    ((0, 0), (0, 1), (3, 0), (-3, 0), (3, 1), (-3, 1)),
    ((1, 0), (-1, 0), (2, 0), (-2, 0)),
    ((4, 0), (4, 1), (2, 1), (-2, 1), (1, 1), (-1, 1)),
)


def local(train_gate, train_up, train_down, router_weight, router_gain):
    z, c = place()
    place_ = jnp.stack([z, c]).astype(jnp.int32)
    ins = (train_gate, train_up, train_down)

    def scratch(n):
        return [
            pltpu.VMEM((n, 3, E, 128, 128), jnp.float32),
            pltpu.SemaphoreType.DMA((n, 3)),
        ]

    def rows_of(n):
        return jax.ShapeDtypeStruct((n, N, 1, 128), jnp.float32)

    nf, nr = len(FIRST), len(REST)
    *sent_first, early = pl.pallas_call(
        first_kernel,
        out_shape=(PIECE,) * (2 * nf) + (rows_of(nf),),
        in_specs=[SMEM, ANY, ANY, ANY],
        out_specs=(VMEM,) * (2 * nf + 1),
        scratch_shapes=scratch(nf),
        name="first",
    )(place_, *ins)
    *sent_rest, table = pl.pallas_call(
        rest_kernel,
        out_shape=(PIECE,) * (2 * nr) + (jax.ShapeDtypeStruct((16, 1, 1280), jnp.float32),),
        in_specs=[SMEM, ANY, ANY, ANY, VMEM, VMEM, VMEM],
        out_specs=(VMEM,) * (2 * nr + 1),
        scratch_shapes=[pltpu.VMEM((nr, N, 1, 128), jnp.float32)] + scratch(nr),
        name="rest",
    )(place_, *ins, early, router_weight.T, router_gain[None])
    sent = {}
    for dzs, pieces in ((FIRST, sent_first), (REST, sent_rest)):
        for i, dz in enumerate(dzs):
            sent[dz, 0], sent[dz, 1] = pieces[2 * i], pieces[2 * i + 1]
    got = {(0, 0): sent[0, 0]}
    for dz, dc in ORDER:
        got[dz, dc] = lax.ppermute(sent[dz, dc], "rows", pairs_of(dz, dc))
    table = lax.all_to_all(table, "rows", 0, 0, tiled=True)
    small = jax.ShapeDtypeStruct((E, 64), jnp.float32)
    scale_gate, scale_up, scale_down, factors, rows = pl.pallas_call(
        scale_kernel,
        out_shape=(small,) * 3
        + (
            jax.ShapeDtypeStruct((16, 128, 8), jnp.float32),
            jax.ShapeDtypeStruct((4, D_MODEL), jnp.bfloat16),
        ),
        in_specs=[VMEM],
        out_specs=(VMEM,) * 5,
        name="scales",
    )(table)
    wide = lax.all_to_all(jnp.broadcast_to(rows[None], (16, 4, D_MODEL)), "owner", 0, 0, tiled=True)
    serve_router = wide.reshape(64, D_MODEL).T
    outs = ()
    for where in GROUPS:
        outs = decode(where, place_, factors, [got[k] for k in where], outs)
    ready_gate, ready_up, ready_down = outs
    return (
        ready_gate.transpose(0, 2, 1),
        ready_up.transpose(0, 2, 1),
        ready_down,
        scale_gate,
        scale_up,
        scale_down,
        serve_router,
    )


def solution(mesh):
    return jax.shard_map(
        local,
        mesh=mesh,
        in_specs=(
            P("owner", "rows", None),
            P("owner", "rows", None),
            P("owner", None, "rows"),
            P("rows", "owner"),
            P("rows"),
        ),
        out_specs=(
            P("owner", None, "rows"),
            P("owner", None, "rows"),
            P("owner", "rows", None),
            P("owner", "rows"),
            P("owner", "rows"),
            P("owner", "rows"),
            P(),
        ),
        check_vma=False,
    )
```

```python
import functools

import jax
import jax.numpy as jnp
from jax import lax
from jax.experimental import pallas as pl
from jax.experimental.pallas import tpu as pltpu
from jax.sharding import PartitionSpec as P


D_MODEL = 2048
E = 4
N = 3 * E
CHIPS = 8
POWER = 13
AMP = 700.0
FLOOR = 1e-25

FIRST = (3, -3)
REST = (1, -1, 2, -2, 4, 0)
ORDER = (
    (3, 0), (-3, 0), (3, 1), (-3, 1), (0, 1), (4, 0), (4, 1), (2, 0), (-2, 0),
    (2, 1), (-2, 1), (1, 0), (-1, 0), (1, 1), (-1, 1),
)


def place():
    r = lax.axis_index("rows")
    return r // 2, r % 2


def pairs_of(dz, dc):
    return [
        (2 * z + c, 2 * ((z + dz) % CHIPS) + (c ^ dc)) for z in range(CHIPS) for c in range(2)
    ]


def code(x, sums):
    v = x * (AMP / jnp.maximum(sums, FLOOR))
    v2 = v * v
    v4 = v2 * v2
    return (v4 * v4 * v4 * v).astype(jnp.bfloat16)


def fetches(dzs, z, ins, buf, sems):
    gate, up, down = ins
    out = []
    for i, dz in enumerate(dzs):
        at = pl.ds(pl.multiple_of(lax.rem(z + (dz % CHIPS), CHIPS) * 128, 128), 128)
        out.append(
            [
                pltpu.make_async_copy(gate.at[:, :, at], buf.at[i, 0], sems.at[i, 0]),
                pltpu.make_async_copy(up.at[:, :, at], buf.at[i, 1], sems.at[i, 1]),
                pltpu.make_async_copy(down.at[:, at, :], buf.at[i, 2], sems.at[i, 2]),
            ]
        )
    return out


def encode(dzs, place_ref, ins, outs, sums, buf, sems):
    z, c = place_ref[0], place_ref[1]
    copies = fetches(dzs, z, ins, buf, sems)
    for three in copies:
        for copy in three:
            copy.start()
    diagonal = lax.broadcasted_iota(jnp.int32, (128, 128), 0) == lax.broadcasted_iota(
        jnp.int32, (128, 128), 1
    )
    mine = c == 0
    for i, three in enumerate(copies):
        same, other = outs[2 * i], outs[2 * i + 1]
        for copy in three:
            copy.wait()

        def put(n, coded):
            low, high = coded[:64], coded[64:]
            same[n] = jnp.where(mine, low, high)
            other[n] = jnp.where(mine, high, low)

        def one(e, carry):
            for a in range(2):
                x = buf[i, a, e]
                total = jnp.sum(jnp.abs(x), axis=0, keepdims=True)
                sums[i, a * E + e] = total
                put(a * E + e, code(x, total).T)
            x = buf[i, 2, e]
            total = jnp.sum(jnp.abs(x), axis=1, keepdims=True)
            sums[i, 2 * E + e] = jnp.sum(jnp.where(diagonal, total, 0.0), axis=0, keepdims=True)
            put(2 * E + e, code(x, total))
            return carry

        lax.fori_loop(0, E, one, 0)


def first_kernel(place_ref, gate, up, down, *rest):
    outs, (sums, buf, sems) = rest[: 2 * len(FIRST)], rest[2 * len(FIRST) :]
    encode(FIRST, place_ref, (gate, up, down), outs, sums, buf, sems)


def rest_kernel(place_ref, gate, up, down, early, router, gain, *rest):
    outs, (table, sums, buf, sems) = rest[: 2 * len(REST)], rest[2 * len(REST) :]
    encode(REST, place_ref, (gate, up, down), outs, sums, buf, sems)
    z = place_ref[0]
    left = lax.broadcasted_iota(jnp.int32, (1, 128), 1) < 64
    served = (router[...] * gain[...]).astype(jnp.bfloat16).astype(jnp.float32)
    for dzs, ref in ((FIRST, early), (REST, sums)):
        for i, dz in enumerate(dzs):
            chip = lax.rem(z + (dz % CHIPS), CHIPS)
            for q in range(N // 2):
                a, b = ref[i, 2 * q], ref[i, 2 * q + 1]
                at = slice(q * 128, q * 128 + 128)
                table[2 * chip, :, at] = jnp.where(left, a, pltpu.roll(b, 64, 1))
                table[2 * chip + 1, :, at] = jnp.where(left, pltpu.roll(a, 64, 1), b)
            for core in range(2):
                for q in range(4):
                    at = slice((N // 2 + q) * 128, (N // 2 + q) * 128 + 128)
                    table[2 * chip + core, :, at] = served[q : q + 1]


def scale_kernel(table, gate, up, down, factors, rows, line):
    total = table[0]
    for s in range(1, 16):
        total = total + table[s]
    scale = total[:, : N // 2 * 128] / D_MODEL
    for n in range(N):
        out = (gate, up, down)[n // E]
        out[n % E : n % E + 1, :] = scale[:, n * 64 : n * 64 + 64]
    for s in range(16):
        f = jnp.maximum(table[s, :, : N // 2 * 128], FLOOR) / (AMP * scale)
        f = [f[:, q * 128 : q * 128 + 128] for q in range(N // 2)]
        factors[s] = jnp.concatenate(f + f[:2], axis=0).T
        for q in range(4):
            at = slice((N // 2 + q) * 128, (N // 2 + q) * 128 + 128)
            line[q : q + 1, s * 128 : s * 128 + 128] = table[s, :, at].astype(jnp.bfloat16)
    for d in range(16):
        rows[d] = line[...]


def decode_kernel(where, n_alias, place_ref, factors, *rest):
    n = len(where)
    pieces, rest = rest[:n], rest[n + n_alias :]
    outs, (buf, sems) = rest[:3], rest[3:]
    z, c = place_ref[0], place_ref[1]
    copies = []
    for i, (dz, dc) in enumerate(where):
        s = 2 * lax.rem(z + (-dz % CHIPS), CHIPS) + (c if dc == 0 else 1 - c)
        f = factors[s]
        for k in range(N):
            w = pieces[i][k].astype(jnp.float32)
            root = jnp.exp(jnp.log(jnp.abs(w)) * (1.0 / POWER))
            root = jnp.where(w < 0, -root, root)
            half = k % 2 * 64
            buf[i, k] = (root * f[half : half + 64, k // 2 : k // 2 + 1]).astype(jnp.bfloat16)
        at = pl.ds(pl.multiple_of(s * 128, 128), 128)
        for a in range(3):
            copy = pltpu.make_async_copy(
                buf.at[i, a * E : a * E + E], outs[a].at[:, :, at], sems.at[i, a]
            )
            copy.start()
            copies.append(copy)
    for copy in copies:
        copy.wait()


SMEM = pl.BlockSpec(memory_space=pltpu.SMEM)
VMEM = pl.BlockSpec(memory_space=pltpu.VMEM)
ANY = pl.BlockSpec(memory_space=pl.ANY)
PIECE = pltpu.VMEM((N, 64, 128), jnp.bfloat16)


def kept(x):
    return pltpu.with_memory_space_constraint(x, pltpu.VMEM)


def decode(where, place_, factors, pieces, before):
    n = len(where)
    out = jax.ShapeDtypeStruct((E, 64, 16 * 128), jnp.bfloat16)
    return pl.pallas_call(
        functools.partial(decode_kernel, where, len(before)),
        out_shape=(out,) * 3,
        in_specs=[SMEM, VMEM] + [VMEM] * n + [ANY] * len(before),
        out_specs=(ANY,) * 3,
        scratch_shapes=[
            pltpu.VMEM((n, N, 64, 128), jnp.bfloat16),
            pltpu.SemaphoreType.DMA((n, 3)),
        ],
        input_output_aliases={2 + n + a: a for a in range(len(before))},
        cost_estimate=pl.CostEstimate(
            flops=n * 10_000_000, transcendentals=0, bytes_accessed=n * 400_000
        ),
    )(place_, kept(factors), *map(kept, pieces), *before)


GROUPS = (
    ((0, 0), (0, 1), (3, 0), (-3, 0), (3, 1), (-3, 1)),
    ((4, 0), (4, 1), (2, 0), (-2, 0)),
    ((2, 1), (-2, 1), (1, 0), (-1, 0)),
    ((1, 1), (-1, 1)),
)


def local(train_gate, train_up, train_down, router_weight, router_gain):
    z, c = place()
    place_ = jnp.stack([z, c]).astype(jnp.int32)
    ins = (train_gate, train_up, train_down)

    def scratch(n):
        return [
            pltpu.VMEM((n, 3, E, 128, 128), jnp.float32),
            pltpu.SemaphoreType.DMA((n, 3)),
        ]

    def rows_of(n):
        return jax.ShapeDtypeStruct((n, N, 1, 128), jnp.float32)

    nf, nr = len(FIRST), len(REST)
    *sent_first, early = pl.pallas_call(
        first_kernel,
        out_shape=(PIECE,) * (2 * nf) + (rows_of(nf),),
        in_specs=[SMEM, ANY, ANY, ANY],
        out_specs=(VMEM,) * (2 * nf + 1),
        scratch_shapes=scratch(nf),
        name="first",
    )(place_, *ins)
    *sent_rest, table = pl.pallas_call(
        rest_kernel,
        out_shape=(PIECE,) * (2 * nr) + (jax.ShapeDtypeStruct((16, 1, 1280), jnp.float32),),
        in_specs=[SMEM, ANY, ANY, ANY, VMEM, VMEM, VMEM],
        out_specs=(VMEM,) * (2 * nr + 1),
        scratch_shapes=[pltpu.VMEM((nr, N, 1, 128), jnp.float32)] + scratch(nr),
        name="rest",
    )(place_, *ins, early, router_weight.T, router_gain[None])
    sent = {}
    for dzs, pieces in ((FIRST, sent_first), (REST, sent_rest)):
        for i, dz in enumerate(dzs):
            sent[dz, 0], sent[dz, 1] = pieces[2 * i], pieces[2 * i + 1]
    got = {(0, 0): sent[0, 0]}
    for dz, dc in ORDER:
        got[dz, dc] = lax.ppermute(sent[dz, dc], "rows", pairs_of(dz, dc))
    table = lax.all_to_all(table, "rows", 0, 0, tiled=True)
    small = jax.ShapeDtypeStruct((E, 64), jnp.float32)
    scale_gate, scale_up, scale_down, factors, rows = pl.pallas_call(
        scale_kernel,
        out_shape=(small,) * 3
        + (
            pltpu.VMEM((16, 128, 8), jnp.float32),
            pltpu.VMEM((16, 4, D_MODEL), jnp.bfloat16),
        ),
        in_specs=[VMEM],
        out_specs=(VMEM,) * 5,
        scratch_shapes=[pltpu.VMEM((4, D_MODEL), jnp.bfloat16)],
        name="scales",
    )(table)
    wide = lax.all_to_all(rows, "owner", 0, 0, tiled=True)
    serve_router = wide.reshape(64, D_MODEL).T
    outs = ()
    for where in GROUPS:
        outs = decode(where, place_, factors, [got[k] for k in where], outs)
    ready_gate, ready_up, ready_down = outs
    return (
        ready_gate.transpose(0, 2, 1),
        ready_up.transpose(0, 2, 1),
        ready_down,
        scale_gate,
        scale_up,
        scale_down,
        serve_router,
    )


def solution(mesh):
    return jax.shard_map(
        local,
        mesh=mesh,
        in_specs=(
            P("owner", "rows", None),
            P("owner", "rows", None),
            P("owner", None, "rows"),
            P("rows", "owner"),
            P("rows"),
        ),
        out_specs=(
            P("owner", None, "rows"),
            P("owner", None, "rows"),
            P("owner", "rows", None),
            P("owner", "rows"),
            P("owner", "rows"),
            P("owner", "rows"),
            P(),
        ),
        check_vma=False,
    )
```

```python
import functools

import jax
import jax.numpy as jnp
from jax import lax
from jax.experimental import pallas as pl
from jax.experimental.pallas import tpu as pltpu
from jax.sharding import PartitionSpec as P


D_MODEL = 2048
E = 4
N = 3 * E
CHIPS = 8
POWER = 13
AMP = 700.0
FLOOR = 1e-25

UNROLL = 2
MiB = 1 << 20
FIRST = (3, -3)
REST = (1, -1, 2, -2, 4, 0)
ORDER = (
    (3, 0), (-3, 0), (3, 1), (-3, 1), (0, 1), (4, 0), (4, 1), (2, 0), (-2, 0),
    (2, 1), (-2, 1), (1, 0), (-1, 0), (1, 1), (-1, 1),
)


def place():
    r = lax.axis_index("rows")
    return lax.shift_right_logical(r, 1), lax.bitwise_and(r, 1)


def pairs_of(dz, dc):
    return [
        (2 * z + c, 2 * ((z + dz) % CHIPS) + (c ^ dc)) for z in range(CHIPS) for c in range(2)
    ]


def code(x, sums):
    v = x * (AMP / jnp.maximum(sums, FLOOR))
    v2 = v * v
    v4 = v2 * v2
    return (v4 * v4 * v4 * v).astype(jnp.bfloat16)


def fetches(dzs, z, ins, buf, sems):
    gate, up, down = ins
    out = []
    for i, dz in enumerate(dzs):
        at = pl.ds(pl.multiple_of(lax.rem(z + (dz % CHIPS), CHIPS) * 128, 128), 128)
        out.append(
            [
                pltpu.make_async_copy(gate.at[:, :, at], buf.at[i, 0], sems.at[i, 0]),
                pltpu.make_async_copy(up.at[:, :, at], buf.at[i, 1], sems.at[i, 1]),
                pltpu.make_async_copy(down.at[:, at, :], buf.at[i, 2], sems.at[i, 2]),
            ]
        )
    return out


def encode(dzs, ins, outs, buf, sems):
    z, c = place()
    copies = fetches(dzs, z, ins, buf, sems)
    for three in copies:
        for copy in three:
            copy.start()
    mine = c == 0
    for i, three in enumerate(copies):
        same, other = outs[2 * i], outs[2 * i + 1]
        for copy in three:
            copy.wait()

        def put(n, coded):
            low, high = coded[:64], coded[64:]
            same[n] = jnp.where(mine, low, high)
            other[n] = jnp.where(mine, high, low)

        def one(e, carry):
            for a in range(2):
                x = buf[i, a, e]
                put(a * E + e, code(x, jnp.sum(jnp.abs(x), axis=0, keepdims=True)).T)
            x = buf[i, 2, e]
            put(2 * E + e, code(x, jnp.sum(jnp.abs(x), axis=1, keepdims=True)))
            return carry

        lax.fori_loop(0, E, one, 0, unroll=UNROLL)


def code_kernel(dzs, gate, up, down, *rest):
    outs, (buf, sems) = rest[: 2 * len(dzs)], rest[2 * len(dzs) :]
    encode(dzs, (gate, up, down), outs, buf, sems)


def sums_kernel(gate, up, down, router, gain, table, buf, tall, line, sems):
    copies = []
    for a, ref in enumerate((gate, up)):
        copies += [pltpu.make_async_copy(ref.at[e], buf.at[a * E + e], sems.at[a * E + e]) for e in range(E)]
    copies += [pltpu.make_async_copy(down.at[e], tall.at[e], sems.at[2 * E + e]) for e in range(E)]
    for copy in copies:
        copy.start()
    diagonal = lax.broadcasted_iota(jnp.int32, (128, 128), 0) == lax.broadcasted_iota(
        jnp.int32, (128, 128), 1
    )
    left = lax.broadcasted_iota(jnp.int32, (8, 128), 1) < 64
    served = (router[...] * gain[...]).astype(jnp.bfloat16).astype(jnp.float32)
    for d in range(16):
        for q in range(4):
            at = slice((N // 2 + q) * 128, (N // 2 + q) * 128 + 128)
            table[d, :, at] = served[q : q + 1]
    for n in range(N):
        q, half = n // 2, n % 2
        copies[n].wait()
        if n < 2 * E:
            line[half, q : q + 1, :] = jnp.sum(jnp.abs(buf[n]), axis=0, keepdims=True)
            continue
        for chip in range(CHIPS):
            at = slice(chip * 128, chip * 128 + 128)
            total = jnp.sum(jnp.abs(tall[n - 2 * E, at]), axis=1, keepdims=True)
            total = jnp.sum(jnp.where(diagonal, total, 0.0), axis=0, keepdims=True)
            line[half, q : q + 1, at] = total
    for chip in range(CHIPS):
        at = slice(chip * 128, chip * 128 + 128)
        a, b = line[0, :, at], line[1, :, at]
        for core, both in enumerate(
            (jnp.where(left, a, pltpu.roll(b, 64, 1)), jnp.where(left, pltpu.roll(a, 64, 1), b))
        ):
            for q in range(N // 2):
                table[2 * chip + core, :, q * 128 : q * 128 + 128] = both[q : q + 1]


def scale_kernel(table, gate, up, down, factors, rows, line):
    total = table[0]
    for s in range(1, 16):
        total = total + table[s]
    scale = total[:, : N // 2 * 128] / D_MODEL
    for n in range(N):
        out = (gate, up, down)[n // E]
        out[n % E : n % E + 1, :] = scale[:, n * 64 : n * 64 + 64]
    for s in range(16):
        f = jnp.maximum(table[s, :, : N // 2 * 128], FLOOR) / (AMP * scale)
        f = [f[:, q * 128 : q * 128 + 128] for q in range(N // 2)]
        factors[s] = jnp.concatenate(f + f[:2], axis=0).T
        for q in range(4):
            at = slice((N // 2 + q) * 128, (N // 2 + q) * 128 + 128)
            line[q : q + 1, s * 128 : s * 128 + 128] = table[s, :, at].astype(jnp.bfloat16)
    for d in range(16):
        rows[d] = line[...]


def decode_kernel(where, n_alias, with_router, factors, *rest):
    n = len(where)
    pieces, rest = rest[:n], rest[n:]
    if with_router:
        wide, rest = rest[0], rest[1:]
    outs, rest = rest[n_alias : n_alias + 3], rest[n_alias + 3 :]
    if with_router:
        served, rest = rest[0], rest[1:]
        for p in range(16):
            served[4 * p : 4 * p + 4, :] = wide[p]
    buf, sems = rest
    z, c = place()
    copies = []
    for i, (dz, dc) in enumerate(where):
        s = 2 * lax.rem(z + (-dz % CHIPS), CHIPS) + (c if dc == 0 else 1 - c)
        f = factors[s]
        for k in range(N):
            w = pieces[i][k].astype(jnp.float32)
            root = jnp.exp(jnp.log(jnp.abs(w)) * (1.0 / POWER))
            root = jnp.where(w < 0, -root, root)
            half = k % 2 * 64
            buf[i, k] = (root * f[half : half + 64, k // 2 : k // 2 + 1]).astype(jnp.bfloat16)
        at = pl.ds(pl.multiple_of(s * 128, 128), 128)
        for a in range(3):
            copy = pltpu.make_async_copy(
                buf.at[i, a * E : a * E + E], outs[a].at[:, :, at], sems.at[i, a]
            )
            copy.start()
            copies.append(copy)
    for copy in copies:
        copy.wait()


VMEM = pl.BlockSpec(memory_space=pltpu.VMEM)
ANY = pl.BlockSpec(memory_space=pl.ANY)
HBM = pl.BlockSpec(memory_space=pltpu.HBM)
PIECE = pltpu.HBM((N, 64, 128), jnp.bfloat16)


def kept(x, where=pltpu.VMEM):
    return pltpu.with_memory_space_constraint(x, where)


def decode(where, factors, pieces, before, wide=None):
    n = len(where)
    out = jax.ShapeDtypeStruct((E, 64, 16 * 128), jnp.bfloat16)
    extra = [] if wide is None else [kept(wide)]
    return pl.pallas_call(
        functools.partial(decode_kernel, where, len(before), wide is not None),
        out_shape=(out,) * 3 + (jax.ShapeDtypeStruct((64, D_MODEL), jnp.bfloat16),) * len(extra),
        in_specs=[VMEM] * (1 + n + len(extra)) + [ANY] * len(before),
        out_specs=(ANY,) * 3 + (VMEM,) * len(extra),
        scratch_shapes=[
            pltpu.VMEM((n, N, 64, 128), jnp.bfloat16),
            pltpu.SemaphoreType.DMA((n, 3)),
        ],
        input_output_aliases={1 + n + len(extra) + a: a for a in range(len(before))},
        cost_estimate=pl.CostEstimate(
            flops=n * 10_000_000, transcendentals=0, bytes_accessed=n * 400_000
        ),
        compiler_params=pltpu.CompilerParams(vmem_limit_bytes=8 * MiB),
    )(kept(factors), *pieces, *extra, *before)


GROUPS = (
    ((0, 0), (0, 1), (3, 0), (-3, 0), (3, 1), (-3, 1)),
    ((4, 0), (4, 1), (2, 0), (-2, 0)),
    ((2, 1), (-2, 1), (1, 0), (-1, 0)),
    ((1, 1), (-1, 1)),
)


def local(train_gate, train_up, train_down, router_weight, router_gain):
    ins = (train_gate, train_up, train_down)
    sent = {}

    def coded(dzs, limit):
        pieces = pl.pallas_call(
            functools.partial(code_kernel, dzs),
            out_shape=(PIECE,) * (2 * len(dzs)),
            in_specs=[HBM, HBM, HBM],
            out_specs=(VMEM,) * (2 * len(dzs)),
            scratch_shapes=[
                pltpu.VMEM((len(dzs), 3, E, 128, 128), jnp.float32),
                pltpu.SemaphoreType.DMA((len(dzs), 3)),
            ],
            compiler_params=pltpu.CompilerParams(vmem_limit_bytes=limit),
        )(*(pltpu.with_memory_space_constraint(x, pltpu.HBM) for x in ins))
        for i, dz in enumerate(dzs):
            sent[dz, 0], sent[dz, 1] = pieces[2 * i], pieces[2 * i + 1]

    coded(FIRST, 6 * MiB)
    table = pl.pallas_call(
        sums_kernel,
        out_shape=pltpu.VMEM((16, 1, 1280), jnp.float32),
        in_specs=[HBM, HBM, HBM, VMEM, VMEM],
        out_specs=VMEM,
        scratch_shapes=[
            pltpu.VMEM((2 * E, 128, 1024), jnp.float32),
            pltpu.VMEM((E, 1024, 128), jnp.float32),
            pltpu.VMEM((2, 8, 1024), jnp.float32),
            pltpu.SemaphoreType.DMA((N,)),
        ],
        compiler_params=pltpu.CompilerParams(vmem_limit_bytes=12 * MiB),
        name="totals",
    )(*ins, router_weight.T, router_gain[None])
    coded(REST, 12 * MiB)
    got = {(0, 0): sent[0, 0]}
    for dz, dc in ORDER:
        got[dz, dc] = lax.ppermute(sent[dz, dc], "rows", pairs_of(dz, dc))
    table = lax.all_to_all(table, "rows", 0, 0, tiled=True)
    small = jax.ShapeDtypeStruct((E, 64), jnp.float32)
    scale_gate, scale_up, scale_down, factors, rows = pl.pallas_call(
        scale_kernel,
        out_shape=(small,) * 3
        + (
            pltpu.VMEM((16, 128, 8), jnp.float32),
            pltpu.VMEM((16, 4, D_MODEL), jnp.bfloat16),
        ),
        in_specs=[VMEM],
        out_specs=(VMEM,) * 5,
        scratch_shapes=[pltpu.VMEM((4, D_MODEL), jnp.bfloat16)],
        compiler_params=pltpu.CompilerParams(vmem_limit_bytes=4 * MiB),
        name="scales",
    )(kept(table))
    wide = lax.all_to_all(rows, "owner", 0, 0, tiled=True)
    outs = ()
    for i, where in enumerate(GROUPS):
        pieces = [kept(got[k], pltpu.HBM if k == (0, 0) else pltpu.VMEM) for k in where]
        outs = decode(where, factors, pieces, outs, wide if i == 2 else None)
        if i == 2:
            *outs, served = outs
    serve_router = served.T
    ready_gate, ready_up, ready_down = outs
    return (
        ready_gate.transpose(0, 2, 1),
        ready_up.transpose(0, 2, 1),
        ready_down,
        scale_gate,
        scale_up,
        scale_down,
        serve_router,
    )


def solution(mesh):
    return jax.shard_map(
        local,
        mesh=mesh,
        in_specs=(
            P("owner", "rows", None),
            P("owner", "rows", None),
            P("owner", None, "rows"),
            P("rows", "owner"),
            P("rows"),
        ),
        out_specs=(
            P("owner", None, "rows"),
            P("owner", None, "rows"),
            P("owner", "rows", None),
            P("owner", "rows"),
            P("owner", "rows"),
            P("owner", "rows"),
            P(),
        ),
        check_vma=False,
    )
```

```python
import functools

import jax
import jax.numpy as jnp
from jax import lax
from jax.experimental import pallas as pl
from jax.experimental.pallas import tpu as pltpu
from jax.sharding import PartitionSpec as P


D_MODEL = 2048
E = 4
N = 3 * E
CHIPS = 8
POWER = 13
AMP = 700.0
FLOOR = 1e-25

UNROLL = 2
MiB = 1 << 20
FIRST = (3, -3)
REST = (1, -1, 2, -2, 4, 0)
ORDER = (
    (3, 0), (-3, 0), (3, 1), (-3, 1), (2, 0), (-2, 0), (0, 1), (4, 0), (4, 1), (2, 1), (-2, 1), (1, 0), (-1, 0), (1, 1), (-1, 1),
)


def place():
    r = lax.axis_index("rows")
    return lax.shift_right_logical(r, 1), lax.bitwise_and(r, 1)


def pairs_of(dz, dc):
    return [
        (2 * z + c, 2 * ((z + dz) % CHIPS) + (c ^ dc)) for z in range(CHIPS) for c in range(2)
    ]


def code(x, sums):
    v = x * (AMP / jnp.maximum(sums, FLOOR))
    v2 = v * v
    v4 = v2 * v2
    return (v4 * v4 * v4 * v).astype(jnp.bfloat16)


def fetches(dzs, z, ins, buf, sems):
    gate, up, down = ins
    out = []
    for i, dz in enumerate(dzs):
        at = pl.ds(pl.multiple_of(lax.rem(z + (dz % CHIPS), CHIPS) * 128, 128), 128)
        out.append(
            [
                pltpu.make_async_copy(gate.at[:, :, at], buf.at[i, 0], sems.at[i, 0]),
                pltpu.make_async_copy(up.at[:, :, at], buf.at[i, 1], sems.at[i, 1]),
                pltpu.make_async_copy(down.at[:, at, :], buf.at[i, 2], sems.at[i, 2]),
            ]
        )
    return out


def encode(dzs, ins, outs, buf, coded, sems, out_sems):
    z, c = place()
    copies = fetches(dzs, z, ins, buf, sems)
    for three in copies:
        for copy in three:
            copy.start()
    mine = c == 0
    sending = []
    for i, three in enumerate(copies):
        same, other = coded.at[2 * i], coded.at[2 * i + 1]
        for copy in three:
            copy.wait()

        def put(n, coded):
            low, high = coded[:64], coded[64:]
            same[n] = jnp.where(mine, low, high)
            other[n] = jnp.where(mine, high, low)

        def one(e, carry):
            for a in range(2):
                x = buf[i, a, e]
                put(a * E + e, code(x, jnp.sum(jnp.abs(x), axis=0, keepdims=True)).T)
            x = buf[i, 2, e]
            put(2 * E + e, code(x, jnp.sum(jnp.abs(x), axis=1, keepdims=True)))
            return carry

        lax.fori_loop(0, E, one, 0, unroll=UNROLL)
        for k in (2 * i, 2 * i + 1):
            copy = pltpu.make_async_copy(coded.at[k], outs[k], out_sems.at[k])
            copy.start()
            sending.append(copy)
    for copy in sending:
        copy.wait()


def code_kernel(dzs, gate, up, down, *rest):
    encode(dzs, (gate, up, down), rest[: 2 * len(dzs)], *rest[2 * len(dzs) :])


def sums_kernel(gate, up, down, router, gain, table, buf, tall, line, sems):
    copies = []
    for a, ref in enumerate((gate, up)):
        copies += [pltpu.make_async_copy(ref.at[e], buf.at[a * E + e], sems.at[a * E + e]) for e in range(E)]
    copies += [pltpu.make_async_copy(down.at[e], tall.at[e], sems.at[2 * E + e]) for e in range(E)]
    for copy in copies:
        copy.start()
    diagonal = lax.broadcasted_iota(jnp.int32, (128, 128), 0) == lax.broadcasted_iota(
        jnp.int32, (128, 128), 1
    )
    left = lax.broadcasted_iota(jnp.int32, (8, 128), 1) < 64
    row = lax.broadcasted_iota(jnp.int32, (8, 128), 0)
    served = (router[...] * gain[...]).astype(jnp.bfloat16).astype(jnp.float32)
    ends = [jnp.where(row == 6, served[k : k + 1], served[k + 1 : k + 2]) for k in (0, 2)]
    for n in range(N):
        q, half = n // 2, n % 2
        copies[n].wait()
        if n < 2 * E:
            line[half, q : q + 1, :] = jnp.sum(jnp.abs(buf[n]), axis=0, keepdims=True)
            continue
        for chip in range(CHIPS):
            at = slice(chip * 128, chip * 128 + 128)
            total = jnp.sum(jnp.abs(tall[n - 2 * E, at]), axis=1, keepdims=True)
            total = jnp.sum(jnp.where(diagonal, total, 0.0), axis=0, keepdims=True)
            line[half, q : q + 1, at] = total
    for chip in range(CHIPS):
        at = slice(chip * 128, chip * 128 + 128)
        a, b = line[0, :, at], line[1, :, at]
        for core, both in enumerate(
            (jnp.where(left, a, pltpu.roll(b, 64, 1)), jnp.where(left, pltpu.roll(a, 64, 1), b))
        ):
            high = both.astype(jnp.bfloat16).astype(jnp.float32)
            parts = (high, both - high)
            parts = [jnp.where(row < N // 2, p, end) for p, end in zip(parts, ends)]
            table[2 * chip + core] = jnp.concatenate(parts, axis=0).astype(jnp.bfloat16)


def scale_kernel(table, gate, up, down, factors, rows, line):
    def sums_of(s):
        parts = table[s].astype(jnp.float32)
        return parts[:8] + parts[8:]

    total = sums_of(0)
    for s in range(1, 16):
        total = total + sums_of(s)
    scale = total / D_MODEL
    for n in range(N):
        out = (gate, up, down)[n // E]
        half = n % 2 * 64
        out[n % E : n % E + 1, :] = scale[n // 2 : n // 2 + 1, half : half + 64]
    for s in range(16):
        factors[s] = (jnp.maximum(sums_of(s), FLOOR) / (AMP * scale)).T
        at = slice(s * 128, s * 128 + 128)
        line[0:2, at] = table[s, 6:8]
        line[2:4, at] = table[s, 14:16]
    for d in range(16):
        rows[d] = line[...]


def decode_kernel(where, n_alias, with_router, factors, *rest):
    n = len(where)
    pieces, rest = rest[:n], rest[n:]
    if with_router:
        wide, rest = rest[0], rest[1:]
    outs, rest = rest[n_alias : n_alias + 3], rest[n_alias + 3 :]
    if with_router:
        served, rest = rest[0], rest[1:]
        for p in range(16):
            served[4 * p : 4 * p + 4, :] = wide[p]
    buf, sems = rest
    z, c = place()
    copies = []
    for i, (dz, dc) in enumerate(where):
        s = 2 * lax.rem(z + (-dz % CHIPS), CHIPS) + (c if dc == 0 else 1 - c)
        f = factors[s]
        for k in range(N):
            w = pieces[i][k].astype(jnp.float32)
            root = jnp.exp(jnp.log(jnp.abs(w)) * (1.0 / POWER))
            root = jnp.where(w < 0, -root, root)
            half = k % 2 * 64
            buf[i, k] = (root * f[half : half + 64, k // 2 : k // 2 + 1]).astype(jnp.bfloat16)
        at = pl.ds(pl.multiple_of(s * 128, 128), 128)
        for a in range(3):
            copy = pltpu.make_async_copy(
                buf.at[i, a * E : a * E + E], outs[a].at[:, :, at], sems.at[i, a]
            )
            copy.start()
            copies.append(copy)
    for copy in copies:
        copy.wait()


VMEM = pl.BlockSpec(memory_space=pltpu.VMEM)
ANY = pl.BlockSpec(memory_space=pl.ANY)
HBM = pl.BlockSpec(memory_space=pltpu.HBM)
PIECE = pltpu.HBM((N, 64, 128), jnp.bfloat16)


def kept(x, where=pltpu.VMEM):
    return pltpu.with_memory_space_constraint(x, where)


def decode(where, factors, pieces, before, wide=None):
    n = len(where)
    out = jax.ShapeDtypeStruct((E, 64, 16 * 128), jnp.bfloat16)
    extra = [] if wide is None else [kept(wide)]
    return pl.pallas_call(
        functools.partial(decode_kernel, where, len(before), wide is not None),
        out_shape=(out,) * 3 + (jax.ShapeDtypeStruct((64, D_MODEL), jnp.bfloat16),) * len(extra),
        in_specs=[VMEM] * (1 + n + len(extra)) + [ANY] * len(before),
        out_specs=(ANY,) * 3 + (VMEM,) * len(extra),
        scratch_shapes=[
            pltpu.VMEM((n, N, 64, 128), jnp.bfloat16),
            pltpu.SemaphoreType.DMA((n, 3)),
        ],
        input_output_aliases={1 + n + len(extra) + a: a for a in range(len(before))},
        cost_estimate=pl.CostEstimate(
            flops=n * 10_000_000, transcendentals=0, bytes_accessed=n * 400_000
        ),
        compiler_params=pltpu.CompilerParams(vmem_limit_bytes=8 * MiB),
    )(kept(factors), *pieces, *extra, *before)


GROUPS = (
    ((0, 0), (0, 1), (3, 0), (-3, 0), (3, 1), (-3, 1)),
    ((2, 0), (-2, 0), (4, 0), (4, 1)),
    ((2, 1), (-2, 1), (1, 0), (-1, 0)),
    ((1, 1),),
    ((-1, 1),),
)


def local(train_gate, train_up, train_down, router_weight, router_gain):
    in_hbm = [kept(x, pltpu.HBM) for x in (train_gate, train_up, train_down)]
    sent = {}

    def coded(dzs, limit):
        pieces = pl.pallas_call(
            functools.partial(code_kernel, dzs),
            out_shape=(PIECE,) * (2 * len(dzs)),
            in_specs=[HBM, HBM, HBM],
            out_specs=(HBM,) * (2 * len(dzs)),
            scratch_shapes=[
                pltpu.VMEM((len(dzs), 3, E, 128, 128), jnp.float32),
                pltpu.VMEM((2 * len(dzs), N, 64, 128), jnp.bfloat16),
                pltpu.SemaphoreType.DMA((len(dzs), 3)),
                pltpu.SemaphoreType.DMA((2 * len(dzs),)),
            ],
            compiler_params=pltpu.CompilerParams(vmem_limit_bytes=limit),
        )(*in_hbm)
        for i, dz in enumerate(dzs):
            sent[dz, 0], sent[dz, 1] = pieces[2 * i], pieces[2 * i + 1]

    coded(FIRST, 6 * MiB)
    table = pl.pallas_call(
        sums_kernel,
        out_shape=pltpu.VMEM((16, 16, 128), jnp.bfloat16),
        in_specs=[HBM, HBM, HBM, VMEM, VMEM],
        out_specs=VMEM,
        scratch_shapes=[
            pltpu.VMEM((2 * E, 128, 1024), jnp.float32),
            pltpu.VMEM((E, 1024, 128), jnp.float32),
            pltpu.VMEM((2, 8, 1024), jnp.float32),
            pltpu.SemaphoreType.DMA((N,)),
        ],
        compiler_params=pltpu.CompilerParams(vmem_limit_bytes=12 * MiB),
        name="totals",
    )(train_gate, train_up, train_down, router_weight.T, router_gain[None])
    coded(REST, 12 * MiB)
    got = {(0, 0): sent[0, 0]}
    for dz, dc in ORDER:
        got[dz, dc] = lax.ppermute(sent[dz, dc], "rows", pairs_of(dz, dc))
    table = lax.all_to_all(table, "rows", 0, 0, tiled=True)
    small = jax.ShapeDtypeStruct((E, 64), jnp.float32)
    scale_gate, scale_up, scale_down, factors, rows = pl.pallas_call(
        scale_kernel,
        out_shape=(small,) * 3
        + (
            pltpu.VMEM((16, 128, 8), jnp.float32),
            pltpu.VMEM((16, 4, D_MODEL), jnp.bfloat16),
        ),
        in_specs=[VMEM],
        out_specs=(VMEM,) * 5,
        scratch_shapes=[pltpu.VMEM((4, D_MODEL), jnp.bfloat16)],
        compiler_params=pltpu.CompilerParams(vmem_limit_bytes=4 * MiB),
        name="scales",
    )(kept(table))
    wide = lax.all_to_all(rows, "owner", 0, 0, tiled=True)
    outs = ()
    for i, where in enumerate(GROUPS):
        pieces = [kept(got[k], pltpu.HBM if k == (0, 0) else pltpu.VMEM) for k in where]
        outs = decode(where, factors, pieces, outs, wide if i == 2 else None)
        if i == 2:
            *outs, served = outs
    serve_router = served.T
    ready_gate, ready_up, ready_down = outs
    return (
        ready_gate.transpose(0, 2, 1),
        ready_up.transpose(0, 2, 1),
        ready_down,
        scale_gate,
        scale_up,
        scale_down,
        serve_router,
    )


def solution(mesh):
    return jax.shard_map(
        local,
        mesh=mesh,
        in_specs=(
            P("owner", "rows", None),
            P("owner", "rows", None),
            P("owner", None, "rows"),
            P("rows", "owner"),
            P("rows"),
        ),
        out_specs=(
            P("owner", None, "rows"),
            P("owner", None, "rows"),
            P("owner", "rows", None),
            P("owner", "rows"),
            P("owner", "rows"),
            P("owner", "rows"),
            P(),
        ),
        check_vma=False,
    )
```

```python
import functools

import jax
import jax.numpy as jnp
from jax import lax
from jax.experimental import pallas as pl
from jax.experimental.pallas import tpu as pltpu
from jax.sharding import PartitionSpec as P


D_MODEL = 2048
E = 4
N = 3 * E
CHIPS = 8
POWER = 13
AMP = 700.0
FLOOR = 1e-25

UNROLL = 2
MiB = 1 << 20
FIRST = (4,)
REST = (3, -3, 2, -2, 1, -1, 0)
ORDER = (
    (4, 0), (4, 1), (3, 0), (-3, 0), (3, 1), (-3, 1), (0, 1), (2, 0), (-2, 0), (2, 1), (-2, 1), (1, 0), (-1, 0), (1, 1), (-1, 1),
)


def place():
    r = lax.axis_index("rows")
    return lax.shift_right_logical(r, 1), lax.bitwise_and(r, 1)


def pairs_of(dz, dc):
    return [
        (2 * z + c, 2 * ((z + dz) % CHIPS) + (c ^ dc)) for z in range(CHIPS) for c in range(2)
    ]


def code(x, sums):
    v = x * (AMP / jnp.maximum(sums, FLOOR))
    v2 = v * v
    v4 = v2 * v2
    return (v4 * v4 * v4 * v).astype(jnp.bfloat16)


def fetches(dzs, z, ins, buf, sems):
    gate, up, down = ins
    out = []
    for i, dz in enumerate(dzs):
        at = pl.ds(pl.multiple_of(lax.rem(z + (dz % CHIPS), CHIPS) * 128, 128), 128)
        out.append(
            [
                pltpu.make_async_copy(gate.at[:, :, at], buf.at[i, 0], sems.at[i, 0]),
                pltpu.make_async_copy(up.at[:, :, at], buf.at[i, 1], sems.at[i, 1]),
                pltpu.make_async_copy(down.at[:, at, :], buf.at[i, 2], sems.at[i, 2]),
            ]
        )
    return out


def encode(dzs, ins, outs, buf, coded, sems, out_sems):
    z, c = place()
    copies = fetches(dzs, z, ins, buf, sems)
    for three in copies:
        for copy in three:
            copy.start()
    mine = c == 0
    sending = []
    for i, three in enumerate(copies):
        same, other = coded.at[2 * i], coded.at[2 * i + 1]
        for copy in three:
            copy.wait()

        def put(n, coded):
            low, high = coded[:64], coded[64:]
            same[n] = jnp.where(mine, low, high)
            other[n] = jnp.where(mine, high, low)

        def one(e, carry):
            for a in range(2):
                x = buf[i, a, e]
                put(a * E + e, code(x, jnp.sum(jnp.abs(x), axis=0, keepdims=True)).T)
            x = buf[i, 2, e]
            put(2 * E + e, code(x, jnp.sum(jnp.abs(x), axis=1, keepdims=True)))
            return carry

        lax.fori_loop(0, E, one, 0, unroll=UNROLL)
        for k in (2 * i, 2 * i + 1):
            copy = pltpu.make_async_copy(coded.at[k], outs[k], out_sems.at[k])
            copy.start()
            sending.append(copy)
    for copy in sending:
        copy.wait()


def code_kernel(dzs, gate, up, down, *rest):
    encode(dzs, (gate, up, down), rest[: 2 * len(dzs)], *rest[2 * len(dzs) :])


def sums_kernel(gate, up, down, router, gain, table, buf, tall, line, sems):
    copies = []
    for a, ref in enumerate((gate, up)):
        copies += [pltpu.make_async_copy(ref.at[e], buf.at[a * E + e], sems.at[a * E + e]) for e in range(E)]
    copies += [pltpu.make_async_copy(down.at[e], tall.at[e], sems.at[2 * E + e]) for e in range(E)]
    for copy in copies:
        copy.start()
    diagonal = lax.broadcasted_iota(jnp.int32, (128, 128), 0) == lax.broadcasted_iota(
        jnp.int32, (128, 128), 1
    )
    left = lax.broadcasted_iota(jnp.int32, (8, 128), 1) < 64
    row = lax.broadcasted_iota(jnp.int32, (8, 128), 0)
    served = (router[...] * gain[...]).astype(jnp.bfloat16).astype(jnp.float32)
    ends = [jnp.where(row == 6, served[k : k + 1], served[k + 1 : k + 2]) for k in (0, 2)]
    for n in range(N):
        q, half = n // 2, n % 2
        copies[n].wait()
        if n < 2 * E:
            line[half, q : q + 1, :] = jnp.sum(jnp.abs(buf[n]), axis=0, keepdims=True)
            continue
        for chip in range(CHIPS):
            at = slice(chip * 128, chip * 128 + 128)
            total = jnp.sum(jnp.abs(tall[n - 2 * E, at]), axis=1, keepdims=True)
            total = jnp.sum(jnp.where(diagonal, total, 0.0), axis=0, keepdims=True)
            line[half, q : q + 1, at] = total
    for chip in range(CHIPS):
        at = slice(chip * 128, chip * 128 + 128)
        a, b = line[0, :, at], line[1, :, at]
        for core, both in enumerate(
            (jnp.where(left, a, pltpu.roll(b, 64, 1)), jnp.where(left, pltpu.roll(a, 64, 1), b))
        ):
            high = both.astype(jnp.bfloat16).astype(jnp.float32)
            parts = (high, both - high)
            parts = [jnp.where(row < N // 2, p, end) for p, end in zip(parts, ends)]
            table[2 * chip + core] = jnp.concatenate(parts, axis=0).astype(jnp.bfloat16)


def scale_kernel(table, gate, up, down, factors, rows, line):
    def sums_of(s):
        parts = table[s].astype(jnp.float32)
        return parts[:8] + parts[8:]

    total = sums_of(0)
    for s in range(1, 16):
        total = total + sums_of(s)
    scale = total / D_MODEL
    for n in range(N):
        out = (gate, up, down)[n // E]
        half = n % 2 * 64
        out[n % E : n % E + 1, :] = scale[n // 2 : n // 2 + 1, half : half + 64]
    for s in range(16):
        factors[s] = (jnp.maximum(sums_of(s), FLOOR) / (AMP * scale)).T
        at = slice(s * 128, s * 128 + 128)
        line[0:2, at] = table[s, 6:8]
        line[2:4, at] = table[s, 14:16]
    for d in range(16):
        rows[d] = line[...]


def decode_kernel(where, n_alias, with_router, factors, *rest):
    n = len(where)
    pieces, rest = rest[:n], rest[n:]
    if with_router:
        wide, rest = rest[0], rest[1:]
    outs, rest = rest[n_alias : n_alias + 3], rest[n_alias + 3 :]
    if with_router:
        served, rest = rest[0], rest[1:]
        for p in range(16):
            served[4 * p : 4 * p + 4, :] = wide[p]
    buf, sems = rest
    z, c = place()
    copies = []
    for i, (dz, dc) in enumerate(where):
        s = 2 * lax.rem(z + (-dz % CHIPS), CHIPS) + (c if dc == 0 else 1 - c)
        f = factors[s]
        for k in range(N):
            w = pieces[i][k].astype(jnp.float32)
            root = jnp.exp(jnp.log(jnp.abs(w)) * (1.0 / POWER))
            root = jnp.where(w < 0, -root, root)
            half = k % 2 * 64
            buf[i, k] = (root * f[half : half + 64, k // 2 : k // 2 + 1]).astype(jnp.bfloat16)
        at = pl.ds(pl.multiple_of(s * 128, 128), 128)
        for a in range(3):
            copy = pltpu.make_async_copy(
                buf.at[i, a * E : a * E + E], outs[a].at[:, :, at], sems.at[i, a]
            )
            copy.start()
            copies.append(copy)
    for copy in copies:
        copy.wait()


VMEM = pl.BlockSpec(memory_space=pltpu.VMEM)
ANY = pl.BlockSpec(memory_space=pl.ANY)
HBM = pl.BlockSpec(memory_space=pltpu.HBM)
PIECE = pltpu.HBM((N, 64, 128), jnp.bfloat16)


def kept(x, where=pltpu.VMEM):
    return pltpu.with_memory_space_constraint(x, where)


def decode(where, factors, pieces, before, wide=None):
    n = len(where)
    out = jax.ShapeDtypeStruct((E, 64, 16 * 128), jnp.bfloat16)
    extra = [] if wide is None else [kept(wide)]
    return pl.pallas_call(
        functools.partial(decode_kernel, where, len(before), wide is not None),
        out_shape=(out,) * 3 + (jax.ShapeDtypeStruct((64, D_MODEL), jnp.bfloat16),) * len(extra),
        in_specs=[VMEM] * (1 + n + len(extra)) + [ANY] * len(before),
        out_specs=(ANY,) * 3 + (VMEM,) * len(extra),
        scratch_shapes=[
            pltpu.VMEM((n, N, 64, 128), jnp.bfloat16),
            pltpu.SemaphoreType.DMA((n, 3)),
        ],
        input_output_aliases={1 + n + len(extra) + a: a for a in range(len(before))},
        cost_estimate=pl.CostEstimate(
            flops=n * 10_000_000, transcendentals=0, bytes_accessed=n * 400_000
        ),
        compiler_params=pltpu.CompilerParams(vmem_limit_bytes=8 * MiB),
    )(kept(factors), *pieces, *extra, *before)


GROUPS = (
    ((0, 0), (0, 1), (4, 0), (4, 1), (3, 0), (-3, 0),),
    ((3, 1), (-3, 1), (2, 0), (-2, 0),),
    ((2, 1), (-2, 1), (1, 0), (-1, 0),),
    ((1, 1),),
    ((-1, 1),),
)


def local(train_gate, train_up, train_down, router_weight, router_gain):
    in_hbm = [kept(x, pltpu.HBM) for x in (train_gate, train_up, train_down)]
    sent = {}

    def coded(dzs, limit):
        pieces = pl.pallas_call(
            functools.partial(code_kernel, dzs),
            out_shape=(PIECE,) * (2 * len(dzs)),
            in_specs=[HBM, HBM, HBM],
            out_specs=(HBM,) * (2 * len(dzs)),
            scratch_shapes=[
                pltpu.VMEM((len(dzs), 3, E, 128, 128), jnp.float32),
                pltpu.VMEM((2 * len(dzs), N, 64, 128), jnp.bfloat16),
                pltpu.SemaphoreType.DMA((len(dzs), 3)),
                pltpu.SemaphoreType.DMA((2 * len(dzs),)),
            ],
            compiler_params=pltpu.CompilerParams(vmem_limit_bytes=limit),
        )(*in_hbm)
        for i, dz in enumerate(dzs):
            sent[dz, 0], sent[dz, 1] = pieces[2 * i], pieces[2 * i + 1]

    coded(FIRST, 6 * MiB)
    table = pl.pallas_call(
        sums_kernel,
        out_shape=pltpu.VMEM((16, 16, 128), jnp.bfloat16),
        in_specs=[HBM, HBM, HBM, VMEM, VMEM],
        out_specs=VMEM,
        scratch_shapes=[
            pltpu.VMEM((2 * E, 128, 1024), jnp.float32),
            pltpu.VMEM((E, 1024, 128), jnp.float32),
            pltpu.VMEM((2, 8, 1024), jnp.float32),
            pltpu.SemaphoreType.DMA((N,)),
        ],
        compiler_params=pltpu.CompilerParams(vmem_limit_bytes=12 * MiB),
        name="totals",
    )(train_gate, train_up, train_down, router_weight.T, router_gain[None])
    coded(REST, 12 * MiB)
    got = {(0, 0): sent[0, 0]}
    for dz, dc in ORDER:
        got[dz, dc] = lax.ppermute(sent[dz, dc], "rows", pairs_of(dz, dc))
    table = lax.all_to_all(table, "rows", 0, 0, tiled=True)
    small = jax.ShapeDtypeStruct((E, 64), jnp.float32)
    scale_gate, scale_up, scale_down, factors, rows = pl.pallas_call(
        scale_kernel,
        out_shape=(small,) * 3
        + (
            pltpu.VMEM((16, 128, 8), jnp.float32),
            pltpu.VMEM((16, 4, D_MODEL), jnp.bfloat16),
        ),
        in_specs=[VMEM],
        out_specs=(VMEM,) * 5,
        scratch_shapes=[pltpu.VMEM((4, D_MODEL), jnp.bfloat16)],
        compiler_params=pltpu.CompilerParams(vmem_limit_bytes=4 * MiB),
        name="scales",
    )(kept(table))
    wide = lax.all_to_all(rows, "owner", 0, 0, tiled=True)
    outs = ()
    for i, where in enumerate(GROUPS):
        pieces = [kept(got[k], pltpu.HBM if k == (0, 0) else pltpu.VMEM) for k in where]
        outs = decode(where, factors, pieces, outs, wide if i == 2 else None)
        if i == 2:
            *outs, served = outs
    serve_router = served.T
    ready_gate, ready_up, ready_down = outs
    return (
        ready_gate.transpose(0, 2, 1),
        ready_up.transpose(0, 2, 1),
        ready_down,
        scale_gate,
        scale_up,
        scale_down,
        serve_router,
    )


def solution(mesh):
    return jax.shard_map(
        local,
        mesh=mesh,
        in_specs=(
            P("owner", "rows", None),
            P("owner", "rows", None),
            P("owner", None, "rows"),
            P("rows", "owner"),
            P("rows"),
        ),
        out_specs=(
            P("owner", None, "rows"),
            P("owner", None, "rows"),
            P("owner", "rows", None),
            P("owner", "rows"),
            P("owner", "rows"),
            P("owner", "rows"),
            P(),
        ),
        check_vma=False,
    )
```

```python
import functools

import jax
import jax.numpy as jnp
from jax import lax
from jax.experimental import pallas as pl
from jax.experimental.pallas import tpu as pltpu
from jax.sharding import PartitionSpec as P


D_MODEL = 2048
E = 4
N = 3 * E
CHIPS = 8
POWER = 13
AMP = 700.0
FLOOR = 1e-25

UNROLL = 2
MiB = 1 << 20
FIRST = (4,)
REST = (3, -3, 2, -2, 1, -1, 0)
ORDER = (
    (4, 0), (4, 1), (2, 0), (-2, 0), (0, 1), (1, 0), (-1, 0), (3, 0), (-3, 0), (1, 1), (-1, 1), (2, 1), (-2, 1), (3, 1), (-3, 1),
)


def place():
    r = lax.axis_index("rows")
    return lax.shift_right_logical(r, 1), lax.bitwise_and(r, 1)


def pairs_of(dz, dc):
    return [
        (2 * z + c, 2 * ((z + dz) % CHIPS) + (c ^ dc)) for z in range(CHIPS) for c in range(2)
    ]


def code(x, sums):
    v = x * (AMP / jnp.maximum(sums, FLOOR))
    v2 = v * v
    v4 = v2 * v2
    return (v4 * v4 * v4 * v).astype(jnp.bfloat16)


def fetches(dzs, z, ins, buf, sems):
    gate, up, down = ins
    out = []
    for i, dz in enumerate(dzs):
        at = pl.ds(pl.multiple_of(lax.rem(z + (dz % CHIPS), CHIPS) * 128, 128), 128)
        out.append(
            [
                pltpu.make_async_copy(gate.at[:, :, at], buf.at[i, 0], sems.at[i, 0]),
                pltpu.make_async_copy(up.at[:, :, at], buf.at[i, 1], sems.at[i, 1]),
                pltpu.make_async_copy(down.at[:, at, :], buf.at[i, 2], sems.at[i, 2]),
            ]
        )
    return out


def encode(dzs, ins, outs, buf, coded, sems, out_sems):
    z, c = place()
    copies = fetches(dzs, z, ins, buf, sems)
    for three in copies:
        for copy in three:
            copy.start()
    mine = c == 0
    sending = []
    for i, three in enumerate(copies):
        same, other = coded.at[2 * i], coded.at[2 * i + 1]
        for copy in three:
            copy.wait()

        def put(n, coded):
            low, high = coded[:64], coded[64:]
            same[n] = jnp.where(mine, low, high)
            other[n] = jnp.where(mine, high, low)

        def one(e, carry):
            for a in range(2):
                x = buf[i, a, e]
                put(a * E + e, code(x, jnp.sum(jnp.abs(x), axis=0, keepdims=True)).T)
            x = buf[i, 2, e]
            put(2 * E + e, code(x, jnp.sum(jnp.abs(x), axis=1, keepdims=True)))
            return carry

        lax.fori_loop(0, E, one, 0, unroll=UNROLL)
        for k in (2 * i, 2 * i + 1):
            copy = pltpu.make_async_copy(coded.at[k], outs[k], out_sems.at[k])
            copy.start()
            sending.append(copy)
    for copy in sending:
        copy.wait()


def code_kernel(dzs, gate, up, down, *rest):
    encode(dzs, (gate, up, down), rest[: 2 * len(dzs)], *rest[2 * len(dzs) :])


def sums_kernel(gate, up, down, router, gain, table, buf, tall, line, sems):
    copies = []
    for a, ref in enumerate((gate, up)):
        copies += [pltpu.make_async_copy(ref.at[e], buf.at[a * E + e], sems.at[a * E + e]) for e in range(E)]
    copies += [pltpu.make_async_copy(down.at[e], tall.at[e], sems.at[2 * E + e]) for e in range(E)]
    for copy in copies:
        copy.start()
    diagonal = lax.broadcasted_iota(jnp.int32, (128, 128), 0) == lax.broadcasted_iota(
        jnp.int32, (128, 128), 1
    )
    left = lax.broadcasted_iota(jnp.int32, (8, 128), 1) < 64
    row = lax.broadcasted_iota(jnp.int32, (8, 128), 0)
    served = (router[...] * gain[...]).astype(jnp.bfloat16).astype(jnp.float32)
    ends = [jnp.where(row == 6, served[k : k + 1], served[k + 1 : k + 2]) for k in (0, 2)]
    for n in range(N):
        q, half = n // 2, n % 2
        copies[n].wait()
        if n < 2 * E:
            line[half, q : q + 1, :] = jnp.sum(jnp.abs(buf[n]), axis=0, keepdims=True)
            continue
        for chip in range(CHIPS):
            at = slice(chip * 128, chip * 128 + 128)
            total = jnp.sum(jnp.abs(tall[n - 2 * E, at]), axis=1, keepdims=True)
            total = jnp.sum(jnp.where(diagonal, total, 0.0), axis=0, keepdims=True)
            line[half, q : q + 1, at] = total
    for chip in range(CHIPS):
        at = slice(chip * 128, chip * 128 + 128)
        a, b = line[0, :, at], line[1, :, at]
        for core, both in enumerate(
            (jnp.where(left, a, pltpu.roll(b, 64, 1)), jnp.where(left, pltpu.roll(a, 64, 1), b))
        ):
            high = both.astype(jnp.bfloat16).astype(jnp.float32)
            parts = (high, both - high)
            parts = [jnp.where(row < N // 2, p, end) for p, end in zip(parts, ends)]
            table[2 * chip + core] = jnp.concatenate(parts, axis=0).astype(jnp.bfloat16)


def scale_kernel(table, gate, up, down, factors, rows, line):
    def sums_of(s):
        parts = table[s].astype(jnp.float32)
        return parts[:8] + parts[8:]

    total = sums_of(0)
    for s in range(1, 16):
        total = total + sums_of(s)
    scale = total / D_MODEL
    for n in range(N):
        out = (gate, up, down)[n // E]
        half = n % 2 * 64
        out[n % E : n % E + 1, :] = scale[n // 2 : n // 2 + 1, half : half + 64]
    for s in range(16):
        factors[s] = (jnp.maximum(sums_of(s), FLOOR) / (AMP * scale)).T
        at = slice(s * 128, s * 128 + 128)
        line[0:2, at] = table[s, 6:8]
        line[2:4, at] = table[s, 14:16]
    for d in range(16):
        rows[d] = line[...]


def decode_kernel(where, n_alias, with_router, factors, *rest):
    n = len(where)
    pieces, rest = rest[:n], rest[n:]
    if with_router:
        wide, rest = rest[0], rest[1:]
    outs, rest = rest[n_alias : n_alias + 3], rest[n_alias + 3 :]
    if with_router:
        served, rest = rest[0], rest[1:]
        for p in range(16):
            served[4 * p : 4 * p + 4, :] = wide[p]
    buf, sems = rest
    z, c = place()
    copies = []
    for i, (dz, dc) in enumerate(where):
        s = 2 * lax.rem(z + (-dz % CHIPS), CHIPS) + (c if dc == 0 else 1 - c)
        f = factors[s]
        for k in range(N):
            w = pieces[i][k].astype(jnp.float32)
            root = jnp.exp(jnp.log(jnp.abs(w)) * (1.0 / POWER))
            root = jnp.where(w < 0, -root, root)
            half = k % 2 * 64
            buf[i, k] = (root * f[half : half + 64, k // 2 : k // 2 + 1]).astype(jnp.bfloat16)
        at = pl.ds(pl.multiple_of(s * 128, 128), 128)
        for a in range(3):
            copy = pltpu.make_async_copy(
                buf.at[i, a * E : a * E + E], outs[a].at[:, :, at], sems.at[i, a]
            )
            copy.start()
            copies.append(copy)
    for copy in copies:
        copy.wait()


VMEM = pl.BlockSpec(memory_space=pltpu.VMEM)
ANY = pl.BlockSpec(memory_space=pl.ANY)
HBM = pl.BlockSpec(memory_space=pltpu.HBM)
PIECE = pltpu.HBM((N, 64, 128), jnp.bfloat16)


def kept(x, where=pltpu.VMEM):
    return pltpu.with_memory_space_constraint(x, where)


def decode(where, factors, pieces, before, wide=None):
    n = len(where)
    out = jax.ShapeDtypeStruct((E, 64, 16 * 128), jnp.bfloat16)
    extra = [] if wide is None else [kept(wide)]
    return pl.pallas_call(
        functools.partial(decode_kernel, where, len(before), wide is not None),
        out_shape=(out,) * 3 + (jax.ShapeDtypeStruct((64, D_MODEL), jnp.bfloat16),) * len(extra),
        in_specs=[VMEM] * (1 + n + len(extra)) + [ANY] * len(before),
        out_specs=(ANY,) * 3 + (VMEM,) * len(extra),
        scratch_shapes=[
            pltpu.VMEM((n, N, 64, 128), jnp.bfloat16),
            pltpu.SemaphoreType.DMA((n, 3)),
        ],
        input_output_aliases={1 + n + len(extra) + a: a for a in range(len(before))},
        cost_estimate=pl.CostEstimate(
            flops=n * 10_000_000, transcendentals=0, bytes_accessed=n * 400_000
        ),
        compiler_params=pltpu.CompilerParams(vmem_limit_bytes=8 * MiB),
    )(kept(factors), *pieces, *extra, *before)


GROUPS = (
    ((0, 0), (0, 1), (4, 0), (4, 1), (2, 0), (-2, 0),),
    ((1, 0), (-1, 0), (3, 0), (-3, 0),),
    ((1, 1), (-1, 1), (2, 1), (-2, 1),),
    ((3, 1),),
    ((-3, 1),),
)


def local(train_gate, train_up, train_down, router_weight, router_gain):
    in_hbm = [kept(x, pltpu.HBM) for x in (train_gate, train_up, train_down)]
    sent = {}

    def coded(dzs, limit):
        pieces = pl.pallas_call(
            functools.partial(code_kernel, dzs),
            out_shape=(PIECE,) * (2 * len(dzs)),
            in_specs=[HBM, HBM, HBM],
            out_specs=(HBM,) * (2 * len(dzs)),
            scratch_shapes=[
                pltpu.VMEM((len(dzs), 3, E, 128, 128), jnp.float32),
                pltpu.VMEM((2 * len(dzs), N, 64, 128), jnp.bfloat16),
                pltpu.SemaphoreType.DMA((len(dzs), 3)),
                pltpu.SemaphoreType.DMA((2 * len(dzs),)),
            ],
            compiler_params=pltpu.CompilerParams(vmem_limit_bytes=limit),
        )(*in_hbm)
        for i, dz in enumerate(dzs):
            sent[dz, 0], sent[dz, 1] = pieces[2 * i], pieces[2 * i + 1]

    coded(FIRST, 6 * MiB)
    table = pl.pallas_call(
        sums_kernel,
        out_shape=pltpu.VMEM((16, 16, 128), jnp.bfloat16),
        in_specs=[HBM, HBM, HBM, VMEM, VMEM],
        out_specs=VMEM,
        scratch_shapes=[
            pltpu.VMEM((2 * E, 128, 1024), jnp.float32),
            pltpu.VMEM((E, 1024, 128), jnp.float32),
            pltpu.VMEM((2, 8, 1024), jnp.float32),
            pltpu.SemaphoreType.DMA((N,)),
        ],
        compiler_params=pltpu.CompilerParams(vmem_limit_bytes=12 * MiB),
        name="totals",
    )(train_gate, train_up, train_down, router_weight.T, router_gain[None])
    coded(REST, 12 * MiB)
    got = {(0, 0): sent[0, 0]}
    for dz, dc in ORDER:
        got[dz, dc] = lax.ppermute(sent[dz, dc], "rows", pairs_of(dz, dc))
    table = lax.all_to_all(table, "rows", 0, 0, tiled=True)
    small = jax.ShapeDtypeStruct((E, 64), jnp.float32)
    scale_gate, scale_up, scale_down, factors, rows = pl.pallas_call(
        scale_kernel,
        out_shape=(small,) * 3
        + (
            pltpu.VMEM((16, 128, 8), jnp.float32),
            pltpu.VMEM((16, 4, D_MODEL), jnp.bfloat16),
        ),
        in_specs=[VMEM],
        out_specs=(VMEM,) * 5,
        scratch_shapes=[pltpu.VMEM((4, D_MODEL), jnp.bfloat16)],
        compiler_params=pltpu.CompilerParams(vmem_limit_bytes=4 * MiB),
        name="scales",
    )(kept(table))
    wide = lax.all_to_all(rows, "owner", 0, 0, tiled=True)
    outs = ()
    for i, where in enumerate(GROUPS):
        pieces = [kept(got[k], pltpu.HBM if k == (0, 0) else pltpu.VMEM) for k in where]
        outs = decode(where, factors, pieces, outs, wide if i == 2 else None)
        if i == 2:
            *outs, served = outs
    serve_router = served.T
    ready_gate, ready_up, ready_down = outs
    return (
        ready_gate.transpose(0, 2, 1),
        ready_up.transpose(0, 2, 1),
        ready_down,
        scale_gate,
        scale_up,
        scale_down,
        serve_router,
    )


def solution(mesh):
    return jax.shard_map(
        local,
        mesh=mesh,
        in_specs=(
            P("owner", "rows", None),
            P("owner", "rows", None),
            P("owner", None, "rows"),
            P("rows", "owner"),
            P("rows"),
        ),
        out_specs=(
            P("owner", None, "rows"),
            P("owner", None, "rows"),
            P("owner", "rows", None),
            P("owner", "rows"),
            P("owner", "rows"),
            P("owner", "rows"),
            P(),
        ),
        check_vma=False,
    )
```

```python
import functools

import jax
import jax.numpy as jnp
from jax import lax
from jax.experimental import pallas as pl
from jax.experimental.pallas import tpu as pltpu
from jax.sharding import PartitionSpec as P


D_MODEL = 2048
E = 4
N = 3 * E
CHIPS = 8
POWER = 13
AMP = 700.0
FLOOR = 1e-25

UNROLL = 2
MiB = 1 << 20
FIRST = (4,)
REST = (3, -3, 2, -2, 1, -1, 0)
ORDER = (
    (4, 0), (4, 1), (2, 0), (-2, 0), (0, 1), (1, 0), (-1, 0), (1, 1), (-1, 1), (2, 1), (-2, 1), (3, 0), (-3, 0), (3, 1), (-3, 1),
)


def place():
    r = lax.axis_index("rows")
    return lax.shift_right_logical(r, 1), lax.bitwise_and(r, 1)


def pairs_of(dz, dc):
    return [
        (2 * z + c, 2 * ((z + dz) % CHIPS) + (c ^ dc)) for z in range(CHIPS) for c in range(2)
    ]


def code(x, sums):
    v = x * (AMP / jnp.maximum(sums, FLOOR))
    v2 = v * v
    v4 = v2 * v2
    return (v4 * v4 * v4 * v).astype(jnp.bfloat16)


def fetches(dzs, z, ins, buf, sems):
    gate, up, down = ins
    out = []
    for i, dz in enumerate(dzs):
        at = pl.ds(pl.multiple_of(lax.rem(z + (dz % CHIPS), CHIPS) * 128, 128), 128)
        out.append(
            [
                pltpu.make_async_copy(gate.at[:, :, at], buf.at[i, 0], sems.at[i, 0]),
                pltpu.make_async_copy(up.at[:, :, at], buf.at[i, 1], sems.at[i, 1]),
                pltpu.make_async_copy(down.at[:, at, :], buf.at[i, 2], sems.at[i, 2]),
            ]
        )
    return out


def encode(dzs, ins, outs, buf, coded, sems, out_sems):
    z, c = place()
    copies = fetches(dzs, z, ins, buf, sems)
    for three in copies:
        for copy in three:
            copy.start()
    mine = c == 0
    sending = []
    for i, three in enumerate(copies):
        same, other = coded.at[2 * i], coded.at[2 * i + 1]
        for copy in three:
            copy.wait()

        def put(n, coded):
            low, high = coded[:64], coded[64:]
            same[n] = jnp.where(mine, low, high)
            other[n] = jnp.where(mine, high, low)

        def one(e, carry):
            for a in range(2):
                x = buf[i, a, e]
                put(a * E + e, code(x, jnp.sum(jnp.abs(x), axis=0, keepdims=True)).T)
            x = buf[i, 2, e]
            put(2 * E + e, code(x, jnp.sum(jnp.abs(x), axis=1, keepdims=True)))
            return carry

        lax.fori_loop(0, E, one, 0, unroll=UNROLL)
        for k in (2 * i, 2 * i + 1):
            copy = pltpu.make_async_copy(coded.at[k], outs[k], out_sems.at[k])
            copy.start()
            sending.append(copy)
    for copy in sending:
        copy.wait()


def code_kernel(dzs, gate, up, down, *rest):
    encode(dzs, (gate, up, down), rest[: 2 * len(dzs)], *rest[2 * len(dzs) :])


def sums_kernel(gate, up, down, router, gain, table, buf, tall, line, sems):
    copies = []
    for a, ref in enumerate((gate, up)):
        copies += [pltpu.make_async_copy(ref.at[e], buf.at[a * E + e], sems.at[a * E + e]) for e in range(E)]
    copies += [pltpu.make_async_copy(down.at[e], tall.at[e], sems.at[2 * E + e]) for e in range(E)]
    for copy in copies:
        copy.start()
    diagonal = lax.broadcasted_iota(jnp.int32, (128, 128), 0) == lax.broadcasted_iota(
        jnp.int32, (128, 128), 1
    )
    left = lax.broadcasted_iota(jnp.int32, (8, 128), 1) < 64
    row = lax.broadcasted_iota(jnp.int32, (8, 128), 0)
    served = (router[...] * gain[...]).astype(jnp.bfloat16).astype(jnp.float32)
    ends = [jnp.where(row == 6, served[k : k + 1], served[k + 1 : k + 2]) for k in (0, 2)]
    for n in range(N):
        q, half = n // 2, n % 2
        copies[n].wait()
        if n < 2 * E:
            line[half, q : q + 1, :] = jnp.sum(jnp.abs(buf[n]), axis=0, keepdims=True)
            continue
        for chip in range(CHIPS):
            at = slice(chip * 128, chip * 128 + 128)
            total = jnp.sum(jnp.abs(tall[n - 2 * E, at]), axis=1, keepdims=True)
            total = jnp.sum(jnp.where(diagonal, total, 0.0), axis=0, keepdims=True)
            line[half, q : q + 1, at] = total
    for chip in range(CHIPS):
        at = slice(chip * 128, chip * 128 + 128)
        a, b = line[0, :, at], line[1, :, at]
        for core, both in enumerate(
            (jnp.where(left, a, pltpu.roll(b, 64, 1)), jnp.where(left, pltpu.roll(a, 64, 1), b))
        ):
            high = both.astype(jnp.bfloat16).astype(jnp.float32)
            parts = (high, both - high)
            parts = [jnp.where(row < N // 2, p, end) for p, end in zip(parts, ends)]
            table[2 * chip + core] = jnp.concatenate(parts, axis=0).astype(jnp.bfloat16)


def scale_kernel(table, gate, up, down, factors, rows, line):
    def sums_of(s):
        parts = table[s].astype(jnp.float32)
        return parts[:8] + parts[8:]

    total = sums_of(0)
    for s in range(1, 16):
        total = total + sums_of(s)
    scale = total / D_MODEL
    for n in range(N):
        out = (gate, up, down)[n // E]
        half = n % 2 * 64
        out[n % E : n % E + 1, :] = scale[n // 2 : n // 2 + 1, half : half + 64]
    for s in range(16):
        factors[s] = (jnp.maximum(sums_of(s), FLOOR) / (AMP * scale)).T
        at = slice(s * 128, s * 128 + 128)
        line[0:2, at] = table[s, 6:8]
        line[2:4, at] = table[s, 14:16]
    for d in range(16):
        rows[d] = line[...]


def decode_kernel(where, n_alias, with_router, factors, *rest):
    n = len(where)
    pieces, rest = rest[:n], rest[n:]
    if with_router:
        wide, rest = rest[0], rest[1:]
    outs, rest = rest[n_alias : n_alias + 3], rest[n_alias + 3 :]
    if with_router:
        served, rest = rest[0], rest[1:]
        for p in range(16):
            served[4 * p : 4 * p + 4, :] = wide[p]
    buf, sems = rest
    z, c = place()
    copies = []
    for i, (dz, dc) in enumerate(where):
        s = 2 * lax.rem(z + (-dz % CHIPS), CHIPS) + (c if dc == 0 else 1 - c)
        f = factors[s]
        for k in range(N):
            w = pieces[i][k].astype(jnp.float32)
            root = jnp.exp(jnp.log(jnp.abs(w)) * (1.0 / POWER))
            root = jnp.where(w < 0, -root, root)
            half = k % 2 * 64
            buf[i, k] = (root * f[half : half + 64, k // 2 : k // 2 + 1]).astype(jnp.bfloat16)
        at = pl.ds(pl.multiple_of(s * 128, 128), 128)
        for a in range(3):
            copy = pltpu.make_async_copy(
                buf.at[i, a * E : a * E + E], outs[a].at[:, :, at], sems.at[i, a]
            )
            copy.start()
            copies.append(copy)
    for copy in copies:
        copy.wait()


VMEM = pl.BlockSpec(memory_space=pltpu.VMEM)
ANY = pl.BlockSpec(memory_space=pl.ANY)
HBM = pl.BlockSpec(memory_space=pltpu.HBM)
PIECE = pltpu.HBM((N, 64, 128), jnp.bfloat16)


def kept(x, where=pltpu.VMEM):
    return pltpu.with_memory_space_constraint(x, where)


def decode(where, factors, pieces, before, wide=None):
    n = len(where)
    out = jax.ShapeDtypeStruct((E, 64, 16 * 128), jnp.bfloat16)
    extra = [] if wide is None else [kept(wide)]
    return pl.pallas_call(
        functools.partial(decode_kernel, where, len(before), wide is not None),
        out_shape=(out,) * 3 + (jax.ShapeDtypeStruct((64, D_MODEL), jnp.bfloat16),) * len(extra),
        in_specs=[VMEM] * (1 + n + len(extra)) + [ANY] * len(before),
        out_specs=(ANY,) * 3 + (VMEM,) * len(extra),
        scratch_shapes=[
            pltpu.VMEM((n, N, 64, 128), jnp.bfloat16),
            pltpu.SemaphoreType.DMA((n, 3)),
        ],
        input_output_aliases={1 + n + len(extra) + a: a for a in range(len(before))},
        cost_estimate=pl.CostEstimate(
            flops=n * 10_000_000, transcendentals=0, bytes_accessed=n * 400_000
        ),
        compiler_params=pltpu.CompilerParams(vmem_limit_bytes=8 * MiB),
    )(kept(factors), *pieces, *extra, *before)


GROUPS = (
    ((0, 0), (0, 1), (4, 0), (4, 1), (2, 0), (-2, 0),),
    ((1, 0), (-1, 0), (1, 1), (-1, 1),),
    ((2, 1), (-2, 1), (3, 0), (-3, 0),),
    ((3, 1),),
    ((-3, 1),),
)


def local(train_gate, train_up, train_down, router_weight, router_gain):
    in_hbm = [kept(x, pltpu.HBM) for x in (train_gate, train_up, train_down)]
    sent = {}

    def coded(dzs, limit):
        pieces = pl.pallas_call(
            functools.partial(code_kernel, dzs),
            out_shape=(PIECE,) * (2 * len(dzs)),
            in_specs=[HBM, HBM, HBM],
            out_specs=(HBM,) * (2 * len(dzs)),
            scratch_shapes=[
                pltpu.VMEM((len(dzs), 3, E, 128, 128), jnp.float32),
                pltpu.VMEM((2 * len(dzs), N, 64, 128), jnp.bfloat16),
                pltpu.SemaphoreType.DMA((len(dzs), 3)),
                pltpu.SemaphoreType.DMA((2 * len(dzs),)),
            ],
            compiler_params=pltpu.CompilerParams(vmem_limit_bytes=limit),
        )(*in_hbm)
        for i, dz in enumerate(dzs):
            sent[dz, 0], sent[dz, 1] = pieces[2 * i], pieces[2 * i + 1]

    coded(FIRST, 6 * MiB)
    table = pl.pallas_call(
        sums_kernel,
        out_shape=pltpu.VMEM((16, 16, 128), jnp.bfloat16),
        in_specs=[HBM, HBM, HBM, VMEM, VMEM],
        out_specs=VMEM,
        scratch_shapes=[
            pltpu.VMEM((2 * E, 128, 1024), jnp.float32),
            pltpu.VMEM((E, 1024, 128), jnp.float32),
            pltpu.VMEM((2, 8, 1024), jnp.float32),
            pltpu.SemaphoreType.DMA((N,)),
        ],
        compiler_params=pltpu.CompilerParams(vmem_limit_bytes=12 * MiB),
        name="totals",
    )(train_gate, train_up, train_down, router_weight.T, router_gain[None])
    coded(REST, 12 * MiB)
    got = {(0, 0): sent[0, 0]}
    for dz, dc in ORDER:
        got[dz, dc] = lax.ppermute(sent[dz, dc], "rows", pairs_of(dz, dc))
    table = lax.all_to_all(table, "rows", 0, 0, tiled=True)
    small = jax.ShapeDtypeStruct((E, 64), jnp.float32)
    scale_gate, scale_up, scale_down, factors, rows = pl.pallas_call(
        scale_kernel,
        out_shape=(small,) * 3
        + (
            pltpu.VMEM((16, 128, 8), jnp.float32),
            pltpu.VMEM((16, 4, D_MODEL), jnp.bfloat16),
        ),
        in_specs=[VMEM],
        out_specs=(VMEM,) * 5,
        scratch_shapes=[pltpu.VMEM((4, D_MODEL), jnp.bfloat16)],
        compiler_params=pltpu.CompilerParams(vmem_limit_bytes=4 * MiB),
        name="scales",
    )(kept(table))
    wide = lax.all_to_all(rows, "owner", 0, 0, tiled=True)
    outs = ()
    for i, where in enumerate(GROUPS):
        pieces = [kept(got[k], pltpu.HBM if k == (0, 0) else pltpu.VMEM) for k in where]
        outs = decode(where, factors, pieces, outs, wide if i == 2 else None)
        if i == 2:
            *outs, served = outs
    serve_router = served.T
    ready_gate, ready_up, ready_down = outs
    return (
        ready_gate.transpose(0, 2, 1),
        ready_up.transpose(0, 2, 1),
        ready_down,
        scale_gate,
        scale_up,
        scale_down,
        serve_router,
    )


def solution(mesh):
    return jax.shard_map(
        local,
        mesh=mesh,
        in_specs=(
            P("owner", "rows", None),
            P("owner", "rows", None),
            P("owner", None, "rows"),
            P("rows", "owner"),
            P("rows"),
        ),
        out_specs=(
            P("owner", None, "rows"),
            P("owner", None, "rows"),
            P("owner", "rows", None),
            P("owner", "rows"),
            P("owner", "rows"),
            P("owner", "rows"),
            P(),
        ),
        check_vma=False,
    )
```
